32 devices in a mesh: dp: 2 (over x), b: 4 (over z), cp: 4 (over y, core).
Axes of the slice: x: 2, y: 2, z: 4, core: 2. Of those that a mesh axis runs over, the one named last changes fastest.
Arguments:
- x: bfloat16 [8, 2048, 2048], P(('dp', 'b'), 'cp'), parts along dimension 0
- ids: int32 [8, 2048, 12], P(('dp', 'b'), 'cp'), parts along dimension 0
- g_attn: bfloat16 [2048], replicated
- wq: bfloat16 [2048, 2048], replicated
- wk: bfloat16 [2048, 2048], replicated
- wv: bfloat16 [2048, 2048], replicated
- wo: bfloat16 [2048, 2048], replicated
- g_ffn: bfloat16 [2048], replicated
- w1: bfloat16 [2048, 8192], replicated
- w3: bfloat16 [2048, 8192], replicated
- w2: bfloat16 [8192, 2048], replicated
- g_moe: bfloat16 [2048], replicated
- wr: bfloat16 [2048, 96], replicated
- we_g: bfloat16 [64, 2048, 1024], P(('b', 'cp'))
- we_u: bfloat16 [64, 2048, 1024], P(('b', 'cp'))
- we_d: bfloat16 [64, 1024, 2048], P(('b', 'cp'))
Outputs:
- output: bfloat16 [8, 2048, 2048], P(('dp', 'b'), 'cp'), parts along dimension 0
There are 2 independent parts. The reference program is written for one: setup_inputs(seed, part) draws one part's arguments, and reference() takes and returns one part's arrays. A program takes and returns all parts, laid end to end along the dimension named above; an argument that names none is the same for every part.
All inputs are finite; a program needn't handle non-finite values.
Results may differ from the reference program's by a relative error of at most 0.00814887.
Values are sent between devices in bfloat16 or wider.
A program may use at most 1 GiB of HBM per device.

```python
import jax
import jax.numpy as jnp
from jax import lax

BATCH = 4
SEQ = 2048
D = 2048
HEADS = 16
KV_HEADS = 16
FF = 8192
EFF = 1024
EXPERTS = 64
ZERO = 32
TOP = 12
NB = 4
NC = 4
HEAD = 128
ROPE = 64
QB = 64
EPS = 1e-6
THETA = 10000.0
RSCALE = 2.5


def rms_norm(x, g):
    xf = x.astype(jnp.float32)
    r = lax.rsqrt(jnp.mean(xf * xf, axis=-1, keepdims=True) + EPS)
    return (xf * r * g.astype(jnp.float32)).astype(jnp.bfloat16)


def rope(t, pos):
    half = ROPE // 2
    freq = THETA ** (-jnp.arange(half, dtype=jnp.float32) / half)
    ang = pos.astype(jnp.float32)[:, None] * freq[None, :]
    c = jnp.cos(ang)[:, None, :]
    s = jnp.sin(ang)[:, None, :]
    tf = t.astype(jnp.float32)
    t1 = tf[..., :half]
    t2 = tf[..., half:ROPE]
    out = jnp.concatenate([t1 * c - t2 * s, t2 * c + t1 * s, tf[..., ROPE:]], axis=-1)
    return out.astype(jnp.bfloat16)


def slot_rank(key):
    n = key.shape[0]
    order = jnp.argsort(key, stable=True)
    sk = key[order]
    first = jnp.searchsorted(sk, sk)
    return jnp.zeros((n,), jnp.int32).at[order].set((jnp.arange(n) - first).astype(jnp.int32))


def setup_inputs(seed: int = 0, part: int = 0) -> dict:
    kg = jax.random.key(seed)
    ks = jax.random.split(kg, 16)
    kp = jax.random.split(jax.random.fold_in(kg, part), 8)
    kz = jax.random.fold_in(kg, 7919)
    kzs = jax.random.split(kz, 2)
    kr = jax.random.split(jax.random.fold_in(kz, part + 1), 4)
    bd = BATCH // NB
    sd = SEQ // NC
    tl = bd * sd
    ns = tl * TOP
    cap = tl * TOP // EXPERTS
    nblk = NB * NC
    nseg = 16

    def w(k, shape, fan, sc):
        return (jax.random.normal(k, shape, jnp.float32) * (sc * fan ** -0.5)).astype(jnp.bfloat16)

    def gain(k):
        return (1.0 + 0.25 * jax.random.normal(k, (D,), jnp.float32)).astype(jnp.bfloat16)

    seg = jnp.arange(SEQ) * nseg // SEQ
    zs = jax.random.normal(kp[0], (BATCH, nseg, D), jnp.float32)
    noise = jax.random.normal(kp[1], (BATCH, SEQ, D), jnp.float32)
    x = (0.8 * zs[:, seg, :] + 0.6 * noise).astype(jnp.bfloat16)

    def limit(raw, zid):
        ffn = raw < EXPERTS
        rank = slot_rank(jnp.where(ffn, raw, EXPERTS))
        return jnp.where(ffn & (rank < cap), raw, zid)

    pop_sum = jnp.sum(jax.random.randint(kzs[0], (EXPERTS, 12), 0, 256), axis=1)
    pop_exp = jnp.clip((pop_sum - 1536) * 277 // 4096 + 64, 0, 127)
    pop_weight = (8 + (pop_exp & 7)) << (pop_exp >> 3)
    pop_cum = jnp.cumsum(pop_weight).astype(jnp.int32)
    zero_limit = jax.random.randint(kr[0], (nblk, tl, 1), 3277, 45876)
    zero_bits = (jax.random.bits(kr[1], (nblk, tl, TOP), jnp.uint32) >> 16).astype(jnp.int32)
    zero_pick = (zero_bits < zero_limit).reshape(nblk, ns)
    pick_draw = jax.random.randint(kr[2], (nblk, ns), 0, pop_cum[-1])
    ffn_id = jnp.minimum(jnp.searchsorted(pop_cum, pick_draw, side='right'), EXPERTS - 1).astype(jnp.int32)
    zero_id = EXPERTS + jax.random.randint(kr[3], (nblk, ns), 0, max(ZERO // 4, 1))
    raw = jnp.where(zero_pick, EXPERTS, ffn_id)
    blk = jax.vmap(limit)(raw, zero_id).astype(jnp.int32)
    ids = blk.reshape(NB, NC, bd, sd, TOP).transpose(0, 2, 1, 3, 4).reshape(BATCH, SEQ, TOP)
    return {
        'x': x,
        'ids': ids,
        'g_attn': gain(ks[0]),
        'wq': w(ks[1], (D, HEADS * HEAD), D, 2.0),
        'wk': w(ks[2], (D, KV_HEADS * HEAD), D, 1.0),
        'wv': w(ks[3], (D, KV_HEADS * HEAD), D, 1.0),
        'wo': w(ks[4], (HEADS * HEAD, D), HEADS * HEAD, 1.0),
        'g_ffn': gain(ks[5]),
        'w1': w(ks[6], (D, FF), D, 1.0),
        'w3': w(ks[7], (D, FF), D, 1.0),
        'w2': w(ks[8], (FF, D), FF, 1.0),
        'g_moe': gain(ks[9]),
        'wr': w(ks[10], (D, EXPERTS + ZERO), D, 1.5),
        'we_g': w(ks[11], (EXPERTS, D, EFF), D, 1.0),
        'we_u': w(ks[12], (EXPERTS, D, EFF), D, 1.0),
        'we_d': w(ks[13], (EXPERTS, EFF, D), EFF, 1.0),
    }


def reference(x, ids, g_attn, wq, wk, wv, wo, g_ffn, w1, w3, w2, g_moe, wr, we_g, we_u, we_d):
    S = x.shape[1]
    pos = jnp.arange(S)
    grp = HEADS // KV_HEADS
    scale = HEAD ** -0.5

    def proj(a, wt):
        return jnp.dot(a, wt, preferred_element_type=jnp.float32).astype(jnp.bfloat16)

    def attn_row(xr):
        n = rms_norm(xr, g_attn)
        q = rope(proj(n, wq).reshape(S, HEADS, HEAD), pos).reshape(S, KV_HEADS, grp, HEAD).astype(jnp.float32)
        k = rope(proj(n, wk).reshape(S, KV_HEADS, HEAD), pos).astype(jnp.float32)
        v = proj(n, wv).reshape(S, KV_HEADS, HEAD).astype(jnp.float32)

        def qblock(i):
            qb = lax.dynamic_slice_in_dim(q, i * QB, QB, axis=0)
            sc = jnp.einsum('qkgd,skd->kgqs', qb, k) * scale
            qp = i * QB + jnp.arange(QB)
            sc = jnp.where(qp[:, None] >= pos[None, :], sc, -jnp.inf)
            p = jax.nn.softmax(sc, axis=-1)
            return jnp.einsum('kgqs,skd->qkgd', p, v)

        o = lax.map(qblock, jnp.arange(S // QB)).reshape(S, HEADS * HEAD).astype(jnp.bfloat16)
        return proj(o, wo)

    a = lax.map(attn_row, x)
    y = (x.astype(jnp.float32) + a.astype(jnp.float32)).astype(jnp.bfloat16)

    def ffn_row(yr):
        z = rms_norm(yr, g_ffn)
        hh = (jax.nn.silu(jnp.dot(z, w1, preferred_element_type=jnp.float32)) * jnp.dot(z, w3, preferred_element_type=jnp.float32)).astype(jnp.bfloat16)
        return proj(hh, w2)

    f = lax.map(ffn_row, y)

    nt = BATCH * S
    N = nt * TOP
    gcap = N // EXPERTS
    u = rms_norm(x, g_moe).reshape(nt, D)
    logits = jnp.dot(u, wr, preferred_element_type=jnp.float32)
    idf = ids.reshape(nt, TOP)
    gate = RSCALE * jax.nn.softmax(jnp.take_along_axis(logits, idf, axis=1), axis=-1)
    e = idf.reshape(N)
    ffn = e < EXPERTS
    ek = jnp.where(ffn, e, EXPERTS)
    slot = jnp.where(ffn, ek * gcap + slot_rank(ek), EXPERTS * gcap)
    us = u[jnp.arange(N) // TOP]
    buf = jnp.zeros((EXPERTS * gcap, D), jnp.bfloat16).at[slot].set(us, mode='drop')

    def expert(args):
        xb, a1, a2, a3 = args
        hh = (jax.nn.silu(jnp.dot(xb, a1, preferred_element_type=jnp.float32)) * jnp.dot(xb, a2, preferred_element_type=jnp.float32)).astype(jnp.bfloat16)
        return proj(hh, a3)

    out = lax.map(expert, (buf.reshape(EXPERTS, gcap, D), we_g, we_u, we_d)).reshape(EXPERTS * gcap, D)
    got = out[jnp.minimum(slot, EXPERTS * gcap - 1)]
    val = jnp.where(ffn[:, None], got.astype(jnp.float32), us.astype(jnp.float32)).reshape(nt, TOP, D)
    m = jnp.einsum('tj,tjd->td', gate, val)
    h = y.astype(jnp.float32) + f.astype(jnp.float32) + m.reshape(BATCH, S, D)
    return h.astype(jnp.bfloat16)
```

```python
import jax
import jax.numpy as jnp
from jax import lax
from jax.sharding import PartitionSpec as P

HEAD = 128
ROPE = 64
EPS = 1e-6
THETA = 10000.0
RSCALE = 2.5


def rms_norm(x, g):
    xf = x.astype(jnp.float32)
    r = lax.rsqrt(jnp.mean(xf * xf, axis=-1, keepdims=True) + EPS)
    return (xf * r * g.astype(jnp.float32)).astype(jnp.bfloat16)


def rope(t, pos):
    half = ROPE // 2
    freq = THETA ** (-jnp.arange(half, dtype=jnp.float32) / half)
    ang = pos.astype(jnp.float32)[:, None] * freq[None, :]
    c = jnp.cos(ang)[:, None, :]
    s = jnp.sin(ang)[:, None, :]
    tf = t.astype(jnp.float32)
    t1 = tf[..., :half]
    t2 = tf[..., half:ROPE]
    out = jnp.concatenate([t1 * c - t2 * s, t2 * c + t1 * s, tf[..., ROPE:]], axis=-1)
    return out.astype(jnp.bfloat16)


def proj(a, wt):
    return jnp.dot(a, wt, preferred_element_type=jnp.float32).astype(jnp.bfloat16)


def swiglu(z, wa, wb, wc):
    hh = (jax.nn.silu(jnp.dot(z, wa, preferred_element_type=jnp.float32)) * jnp.dot(z, wb, preferred_element_type=jnp.float32)).astype(jnp.bfloat16)
    return proj(hh, wc)


def attend(q, kb, vb, qpos, kpos, mx, den, acc):
    s = jnp.einsum('bkgqd,bskd->bkgqs', q, kb, preferred_element_type=jnp.float32) * (HEAD ** -0.5)
    s = jnp.where(qpos[:, None] >= kpos[None, :], s, -1e30)
    mnew = jnp.maximum(mx, jnp.max(s, axis=-1))
    corr = jnp.exp(mx - mnew)
    p = jnp.exp(s - mnew[..., None])
    den = den * corr + jnp.sum(p, axis=-1)
    pv = jnp.einsum('bkgqs,bskd->bkgqd', p.astype(jnp.bfloat16), vb, preferred_element_type=jnp.float32)
    acc = acc * corr[..., None] + pv
    return mnew, den, acc


CAP = 96


def gates(u, ids, wr, nexp):
    t = u.shape[0]
    top = ids.shape[-1]
    logits = jnp.dot(u, wr, preferred_element_type=jnp.float32)
    idf = ids.reshape(t, top)
    cols = jnp.arange(logits.shape[1])
    pick = idf[:, :, None] == cols[None, None, :]
    gate = RSCALE * jax.nn.softmax(jnp.sum(jnp.where(pick, logits[:, None, :], 0.0), axis=-1), axis=-1)
    gsum = jnp.sum(jnp.where(pick, gate[..., None], 0.0), axis=1)
    have = jnp.any(pick, axis=1)
    zero = jnp.sum(gsum[:, nexp:], axis=-1, keepdims=True)
    table = jnp.where(have, gsum, -1.0)[:, :nexp]
    return table.T, zero


def split3(g):
    hi = g.astype(jnp.bfloat16)
    r = g - hi.astype(jnp.float32)
    mid = r.astype(jnp.bfloat16)
    lo = (r - mid.astype(jnp.float32)).astype(jnp.bfloat16)
    return hi, mid, lo


def moe_partials(uall, tab, we_g, we_u, we_d, nchunk):
    ndev, t, d = uall.shape
    epd = we_g.shape[0]
    have = tab >= 0.0
    ti = jnp.arange(t)
    lower = (ti[:, None] < ti[None, :]).astype(jnp.bfloat16)
    rank = jnp.einsum('set,tr->ser', have.astype(jnp.bfloat16), lower, preferred_element_type=jnp.float32)
    rank = jnp.where(have, rank, -1.0)
    sel = rank[:, :, None, :] == jnp.arange(CAP, dtype=jnp.float32)[None, None, :, None]
    selb = sel.astype(jnp.bfloat16).reshape(ndev, epd * CAP, t)
    xin = jnp.einsum('sct,std->scd', selb, uall, preferred_element_type=jnp.float32).astype(jnp.bfloat16)
    xin = xin.reshape(ndev, epd, CAP, d).transpose(1, 0, 2, 3).reshape(epd, ndev * CAP, d)
    hg = jnp.einsum('ecd,edf->ecf', xin, we_g, preferred_element_type=jnp.float32)
    hu = jnp.einsum('ecd,edf->ecf', xin, we_u, preferred_element_type=jnp.float32)
    hh = (jax.nn.silu(hg) * hu).astype(jnp.bfloat16)
    parts = [jnp.where(sel, p[:, :, None, :], jnp.zeros((), jnp.bfloat16)).reshape(ndev, epd * CAP, t) for p in split3(tab)]
    comb = jnp.concatenate(parts, axis=1)
    outs = []
    w = d // nchunk
    for i in range(nchunk):
        yo = jnp.einsum('ecf,efd->ecd', hh, we_d[:, :, i * w:(i + 1) * w], preferred_element_type=jnp.float32).astype(jnp.bfloat16)
        yo = yo.reshape(epd, ndev, CAP, w).transpose(1, 0, 2, 3).reshape(ndev, epd * CAP, w)
        y3 = jnp.concatenate([yo, yo, yo], axis=1)
        part = jnp.einsum('sct,scd->std', comb, y3, preferred_element_type=jnp.float32)
        outs.append(part.reshape(ndev * t, w))
    return outs


NCHUNK = 2


def solution(mesh):
    ncp = mesh.shape['cp']
    ndev = mesh.shape['b'] * ncp
    tok = P(('dp', 'b'), 'cp', None)
    rep = P()
    exs = P(('b', 'cp'), None, None)

    def body(x, ids, g_attn, wq, wk, wv, wo, g_ffn, w1, w3, w2, g_moe, wr, we_g, we_u, we_d):
        bd, sd, d = x.shape
        nh = wq.shape[1] // HEAD
        nexp = we_g.shape[0] * ndev
        u = rms_norm(x, g_moe).reshape(bd * sd, d)
        uall = lax.all_gather(u, ('b', 'cp'), axis=0, tiled=False)
        tab, zero = gates(u, ids, wr, nexp)
        tall = lax.all_gather(tab, ('b', 'cp'), axis=0, tiled=False)
        ci = lax.axis_index('cp')
        epd = we_g.shape[0]
        e0 = (lax.axis_index('b') * ncp + ci) * epd
        tall = lax.dynamic_slice_in_dim(tall, e0, epd, axis=1)
        pos = ci * sd + jnp.arange(sd)
        n = rms_norm(x, g_attn)
        q = rope(proj(n, wq).reshape(bd, sd, nh, HEAD), pos).reshape(bd, sd, nh, 1, HEAD).transpose(0, 2, 3, 1, 4)
        kv = jnp.stack([rope(proj(n, wk).reshape(bd, sd, nh, HEAD), pos), proj(n, wv).reshape(bd, sd, nh, HEAD)])
        mx = jnp.full((bd, nh, 1, sd), -1e30, jnp.float32)
        den = jnp.zeros((bd, nh, 1, sd), jnp.float32)
        acc = jnp.zeros((bd, nh, 1, sd, HEAD), jnp.float32)
        mx, den, acc = attend(q, kv[0], kv[1], pos, pos, mx, den, acc)
        for step in range(1, ncp):
            kv = lax.ppermute(kv, 'cp', [(j, j + 1) for j in range(step - 1, ncp - 1)])
            kpos = ((ci - step) % ncp) * sd + jnp.arange(sd)
            mx, den, acc = attend(q, kv[0], kv[1], pos, kpos, mx, den, acc)
        o = (acc / den[..., None]).astype(jnp.bfloat16).transpose(0, 3, 1, 2, 4).reshape(bd, sd, nh * HEAD)
        y = (x.astype(jnp.float32) + proj(o, wo).astype(jnp.float32)).astype(jnp.bfloat16)
        parts = moe_partials(uall, tall, we_g, we_u, we_d, NCHUNK)
        y, parts = lax.optimization_barrier((y, parts))
        ms = [lax.psum_scatter(p, ('b', 'cp'), scatter_dimension=0, tiled=True) for p in parts]
        f = swiglu(rms_norm(y, g_ffn), w1, w3, w2)
        base = y.astype(jnp.float32) + f.astype(jnp.float32)
        m = jnp.concatenate(ms, axis=1) + zero * u.astype(jnp.float32)
        h = base + m.reshape(bd, sd, d)
        return h.astype(jnp.bfloat16)

    return jax.shard_map(body, mesh=mesh, in_specs=(tok, tok, rep, rep, rep, rep, rep, rep, rep, rep, rep, rep, rep, exs, exs, exs), out_specs=tok, check_vma=False)
```

```python
import jax
import jax.numpy as jnp
from jax import lax
from jax.sharding import PartitionSpec as P


HEAD = 128
ROPE = 64
EPS = 1e-6
THETA = 10000.0
RSCALE = 2.5


def rms_norm(x, g):
    xf = x.astype(jnp.float32)
    r = lax.rsqrt(jnp.mean(xf * xf, axis=-1, keepdims=True) + EPS)
    return (xf * r * g.astype(jnp.float32)).astype(jnp.bfloat16)


def rope(t, pos):
    half = ROPE // 2
    freq = THETA ** (-jnp.arange(half, dtype=jnp.float32) / half)
    ang = pos.astype(jnp.float32)[:, None] * freq[None, :]
    c = jnp.cos(ang)[:, None, :]
    s = jnp.sin(ang)[:, None, :]
    tf = t.astype(jnp.float32)
    t1 = tf[..., :half]
    t2 = tf[..., half:ROPE]
    out = jnp.concatenate([t1 * c - t2 * s, t2 * c + t1 * s, tf[..., ROPE:]], axis=-1)
    return out.astype(jnp.bfloat16)


def proj(a, wt):
    return jnp.dot(a, wt, preferred_element_type=jnp.float32).astype(jnp.bfloat16)


def attend(q, kb, vb, qpos, kpos, mx, den, acc):
    s = jnp.einsum('bkgqd,bskd->bkgqs', q, kb, preferred_element_type=jnp.float32) * (HEAD ** -0.5)
    s = jnp.where(qpos[:, None] >= kpos[None, :], s, -1e30)
    mnew = jnp.maximum(mx, jnp.max(s, axis=-1))
    corr = jnp.exp(mx - mnew)
    p = jnp.exp(s - mnew[..., None])
    den = den * corr + jnp.sum(p, axis=-1)
    pv = jnp.einsum('bkgqs,bskd->bkgqd', p.astype(jnp.bfloat16), vb, preferred_element_type=jnp.float32)
    acc = acc * corr[..., None] + pv
    return mnew, den, acc


CAP = 96
ORDER = ((3, 2, 1, 0), (0, 3, 2, 1), (3, 0, 1, 2), (0, 1, 2, 3))


def gates(u, ids, wr, nexp):
    t = u.shape[0]
    top = ids.shape[-1]
    logits = jnp.dot(u, wr, preferred_element_type=jnp.float32)
    idf = ids.reshape(t, top)
    pick = idf[:, :, None] == jnp.arange(logits.shape[1])[None, None, :]
    gate = RSCALE * jax.nn.softmax(jnp.sum(jnp.where(pick, logits[:, None, :], 0.0), axis=-1), axis=-1)
    zero = jnp.sum(jnp.where(idf >= nexp, gate, 0.0), axis=-1, keepdims=True)
    return jnp.concatenate([idf.astype(jnp.float32), gate], axis=1).T, zero


def tables(info, first, count):
    top = info.shape[1] // 2
    t = info.shape[2]
    ex = (first + jnp.arange(count)).astype(jnp.float32)[None, :, None]
    g = jnp.zeros((info.shape[0], count, t), jnp.float32)
    have = jnp.zeros((info.shape[0], count, t), jnp.bool_)
    for j in range(top):
        hit = info[:, j:j + 1, :] == ex
        g = g + jnp.where(hit, info[:, top + j:top + j + 1, :], 0.0)
        have = have | hit
    ti = jnp.arange(t)
    before = (ti[:, None] < ti[None, :]).astype(jnp.bfloat16)
    rank = jnp.einsum('set,tr->ser', have.astype(jnp.bfloat16), before, preferred_element_type=jnp.float32)
    return g, jnp.where(have, rank, -1.0).astype(jnp.bfloat16)


def split3(g):
    hi = g.astype(jnp.bfloat16)
    r = g - hi.astype(jnp.float32)
    mid = r.astype(jnp.bfloat16)
    lo = (r - mid.astype(jnp.float32)).astype(jnp.bfloat16)
    return hi, mid, lo


def pick_rows(rank):
    epd = rank.shape[1]
    r = jnp.arange(epd * CAP)
    rep = (r[:, None] // CAP == jnp.arange(epd)[None, :]).astype(jnp.bfloat16)
    full = jnp.einsum('re,set->srt', rep, rank, preferred_element_type=jnp.float32)
    return (full == (r % CAP).astype(jnp.float32)[None, :, None]).astype(jnp.bfloat16)


def expert_rows(ublk, sel, we_g, we_u, we_d):
    n, _, d = ublk.shape
    epd = we_g.shape[0]
    xin = jnp.einsum('srt,std->srd', sel, ublk, preferred_element_type=jnp.float32).astype(jnp.bfloat16)
    xin = xin.reshape(n, epd, CAP, d).transpose(1, 0, 2, 3).reshape(epd, n * CAP, d)
    hg = jnp.einsum('ecd,edf->ecf', xin, we_g, preferred_element_type=jnp.float32)
    hu = jnp.einsum('ecd,edf->ecf', xin, we_u, preferred_element_type=jnp.float32)
    hh = lax.optimization_barrier((jax.nn.silu(hg) * hu).astype(jnp.bfloat16))
    yo = jnp.einsum('ecf,efd->ecd', hh, we_d, preferred_element_type=jnp.float32).astype(jnp.bfloat16)
    return yo.reshape(epd, n, CAP, d)


def weights(g, rank):
    ne, _ = g.shape
    r = jnp.arange(ne * CAP)
    rep = (r[:, None] // CAP == jnp.arange(ne)[None, :]).astype(jnp.bfloat16)
    full = jnp.einsum('et,re->tr', rank, rep, preferred_element_type=jnp.float32)
    sel = (full == (r % CAP).astype(jnp.float32)[None, :])[None]
    w = jnp.einsum('pet,re->ptr', jnp.stack(split3(g)), rep, preferred_element_type=jnp.float32)
    return jnp.where(sel, w, 0.0).astype(jnp.bfloat16)


def solution(mesh):
    ncp = mesh.shape['cp']
    ndev = mesh.shape['b'] * ncp
    tok = P(('dp', 'b'), 'cp', None)
    rep = P()
    exs = P(('b', 'cp'), None, None)

    def layer(x, ids, g_attn, wq, wk, wv, wo, g_ffn, w1, w3, w2, g_moe, wr, we_g, we_u, we_d):
        bd, sd, d = x.shape
        nh = wq.shape[1] // HEAD
        epd = we_g.shape[0]
        nexp = epd * ndev
        nb = ndev // ncp
        ci = lax.axis_index('cp')
        bi = lax.axis_index('b')
        u = rms_norm(x, g_moe).reshape(bd * sd, d)
        uall = lax.all_gather(u, ('b', 'cp'), axis=0, tiled=False)
        info, zero = gates(u, ids, wr, nexp)
        info = lax.all_gather(info, ('b', 'cp'), axis=0, tiled=False)
        pos = ci * sd + jnp.arange(sd)
        n = rms_norm(x, g_attn)
        q = rope(proj(n, wq).reshape(bd, sd, nh, HEAD), pos).reshape(bd, sd, nh, 1, HEAD).transpose(0, 2, 3, 1, 4)
        kv = jnp.stack([rope(proj(n, wk).reshape(bd, sd, nh, HEAD), pos), proj(n, wv).reshape(bd, sd, nh, HEAD)])
        mx = jnp.full((bd, nh, 1, sd), -1e30, jnp.float32)
        den = jnp.zeros((bd, nh, 1, sd), jnp.float32)
        acc = jnp.zeros((bd, nh, 1, sd, HEAD), jnp.float32)
        mx, den, acc = attend(q, kv[0], kv[1], pos, pos, mx, den, acc)
        for step in range(1, ncp):
            kv = lax.ppermute(kv, 'cp', [(j, j + 1) for j in range(step - 1, ncp - 1)])
            kpos = ((ci - step) % ncp) * sd + jnp.arange(sd)
            mx, den, acc = attend(q, kv[0], kv[1], pos, kpos, mx, den, acc)
        o = (acc / den[..., None]).astype(jnp.bfloat16).transpose(0, 3, 1, 2, 4).reshape(bd, sd, nh * HEAD)
        y = (x.astype(jnp.float32) + proj(o, wo).astype(jnp.float32)).astype(jnp.bfloat16)

        g, rank = tables(info, bi * (ncp * epd), ncp * epd)
        g = g.reshape(nb, ncp, ncp * epd, sd)
        rank = rank.reshape(nb, ncp, ncp * epd, sd)
        mine = lax.dynamic_slice_in_dim(rank, ci * epd, epd, axis=2)
        gcol = lax.dynamic_index_in_dim(g, ci, axis=1, keepdims=False)
        rcol = lax.dynamic_index_in_dim(rank, ci, axis=1, keepdims=False)
        peers = [jnp.bitwise_xor(ci, k) for k in range(ncp)]
        order = jnp.asarray(ORDER, jnp.int32)
        blks = [order[bi, i] for i in range(nb)]
        uall = uall.reshape(nb, ncp, sd, d)

        def row_picks(i):
            return pick_rows(lax.dynamic_index_in_dim(mine, blks[i], axis=0, keepdims=False))

        def row_weights(i):
            gi = lax.dynamic_index_in_dim(gcol, blks[i], axis=0, keepdims=False)
            ri = lax.dynamic_index_in_dim(rcol, blks[i], axis=0, keepdims=False)
            gi = jnp.concatenate([lax.dynamic_slice_in_dim(gi, p * epd, epd, axis=0) for p in peers], axis=0)
            ri = jnp.concatenate([lax.dynamic_slice_in_dim(ri, p * epd, epd, axis=0) for p in peers], axis=0)
            return weights(gi, ri).reshape(3 * sd, ncp * epd * CAP)

        def work(ua, i):
            blk = lax.dynamic_index_in_dim(ua, blks[i], axis=0, keepdims=False)
            return expert_rows(blk, sels[i], we_g, we_u, we_d)

        def send(yo):
            got = []
            for k in range(ncp):
                part = lax.dynamic_index_in_dim(yo, peers[k], axis=1, keepdims=False).reshape(epd * CAP, d)
                if k:
                    part = lax.ppermute(part, 'cp', [(j, j ^ k) for j in range(ncp)])
                got.append(part)
            return got

        def total(got, i):
            rows = lax.optimization_barrier(jnp.concatenate(got, axis=0))
            p = lax.optimization_barrier(jnp.dot(ws[i], rows, preferred_element_type=jnp.float32)).reshape(3, sd, d)
            return p[0] + p[1] + p[2]

        tie = lax.optimization_barrier

        def up(v, step):
            return lax.ppermute(v, 'b', [(j, j + 1) for j in range(step)])

        def down(v, step):
            return lax.ppermute(v, 'b', [(nb - 1 - j, nb - 2 - j) for j in range(step)])

        sels = tie([row_picks(i) for i in range(nb)])
        ws = tie([row_weights(i) for i in range(nb)])
        uall, y, sels, ws = tie((uall, y, sels, ws))
        yo1, uall = tie((work(uall, 0), uall))
        g1 = send(yo1)
        yo2, uall, g1[0] = tie((work(uall, 1), uall, g1[0]))
        g2 = send(yo2)
        p1, uall = tie((total(g1, 0), uall))
        up1, dn1 = up(p1, 1), down(p1, 1)
        yo3, uall, g2[0] = tie((work(uall, 2), uall, g2[0]))
        g3 = send(yo3)
        p2, uall = tie((total(g2, 1), uall))
        yo4, g3[0] = tie((work(uall, 3), g3[0]))
        g4 = send(yo4)
        a2, b2 = p2 + up1, p2 + dn1
        p3, a2, b2, y = tie((total(g3, 2), a2, b2, y))
        up2, dn2 = up(a2, 2), down(b2, 2)
        zf = rms_norm(y, g_ffn)
        hh = (jax.nn.silu(jnp.dot(zf, w1, preferred_element_type=jnp.float32)) * jnp.dot(zf, w3, preferred_element_type=jnp.float32)).astype(jnp.bfloat16)
        a3 = jnp.where(bi == 2, p1, p3) + up2
        b3 = jnp.where(bi == 1, p1, p3) + dn2
        hh, a3, b3, g4[0] = tie((hh, a3, b3, g4[0]))
        up3, dn3 = up(a3, 3), down(b3, 3)
        p4 = total(g4, 3)
        f = proj(hh, w2)
        m = (p4 + zero * u.astype(jnp.float32)) + up3 + dn3
        h = y.astype(jnp.float32) + f.astype(jnp.float32) + m.reshape(bd, sd, d)
        return h.astype(jnp.bfloat16)

    return jax.shard_map(layer, mesh=mesh, in_specs=(tok, tok, rep, rep, rep, rep, rep, rep, rep, rep, rep, rep, rep, exs, exs, exs), out_specs=tok, check_vma=False)
```

```python
import jax
import jax.numpy as jnp
from jax import lax
from jax.sharding import PartitionSpec as P


HEAD = 128
ROPE = 64
EPS = 1e-6
THETA = 10000.0
RSCALE = 2.5


def rms_norm(x, g):
    xf = x.astype(jnp.float32)
    r = lax.rsqrt(jnp.mean(xf * xf, axis=-1, keepdims=True) + EPS)
    return (xf * r * g.astype(jnp.float32)).astype(jnp.bfloat16)


def rope(t, pos):
    half = ROPE // 2
    freq = THETA ** (-jnp.arange(half, dtype=jnp.float32) / half)
    ang = pos.astype(jnp.float32)[:, None] * freq[None, :]
    c = jnp.cos(ang)[:, None, :]
    s = jnp.sin(ang)[:, None, :]
    tf = t.astype(jnp.float32)
    t1 = tf[..., :half]
    t2 = tf[..., half:ROPE]
    out = jnp.concatenate([t1 * c - t2 * s, t2 * c + t1 * s, tf[..., ROPE:]], axis=-1)
    return out.astype(jnp.bfloat16)


def proj(a, wt):
    return jnp.dot(a, wt, preferred_element_type=jnp.float32).astype(jnp.bfloat16)


def attend(q, kb, vb, qpos, kpos, mx, den, acc):
    s = jnp.einsum('bkgqd,bskd->bkgqs', q, kb, preferred_element_type=jnp.float32) * (HEAD ** -0.5)
    s = jnp.where(qpos[:, None] >= kpos[None, :], s, -1e30)
    mnew = jnp.maximum(mx, jnp.max(s, axis=-1))
    corr = jnp.exp(mx - mnew)
    p = jnp.exp(s - mnew[..., None])
    den = den * corr + jnp.sum(p, axis=-1)
    pv = jnp.einsum('bkgqs,bskd->bkgqd', p.astype(jnp.bfloat16), vb, preferred_element_type=jnp.float32)
    acc = acc * corr[..., None] + pv
    return mnew, den, acc


CAP = 96
ORDER = ((3, 2, 1, 0), (0, 3, 2, 1), (3, 0, 1, 2), (0, 1, 2, 3))


def gates(u, ids, wr, nexp):
    t = u.shape[0]
    top = ids.shape[-1]
    logits = jnp.dot(u, wr, preferred_element_type=jnp.float32)
    idf = ids.reshape(t, top)
    pick = idf[:, :, None] == jnp.arange(logits.shape[1])[None, None, :]
    gate = RSCALE * jax.nn.softmax(jnp.sum(jnp.where(pick, logits[:, None, :], 0.0), axis=-1), axis=-1)
    zero = jnp.sum(jnp.where(idf >= nexp, gate, 0.0), axis=-1, keepdims=True)
    return jnp.concatenate([idf.astype(jnp.float32), gate], axis=1).T, zero


def tables(info, first, count):
    top = info.shape[1] // 2
    t = info.shape[2]
    ex = (first + jnp.arange(count)).astype(jnp.float32)[None, :, None]
    g = jnp.zeros((info.shape[0], count, t), jnp.float32)
    have = jnp.zeros((info.shape[0], count, t), jnp.bool_)
    for j in range(top):
        hit = info[:, j:j + 1, :] == ex
        g = g + jnp.where(hit, info[:, top + j:top + j + 1, :], 0.0)
        have = have | hit
    ti = jnp.arange(t)
    before = (ti[:, None] < ti[None, :]).astype(jnp.bfloat16)
    rank = jnp.einsum('set,tr->ser', have.astype(jnp.bfloat16), before, preferred_element_type=jnp.float32)
    return g, jnp.where(have, rank, -1.0).astype(jnp.bfloat16)


def split3(g):
    hi = g.astype(jnp.bfloat16)
    r = g - hi.astype(jnp.float32)
    mid = r.astype(jnp.bfloat16)
    lo = (r - mid.astype(jnp.float32)).astype(jnp.bfloat16)
    return hi, mid, lo


def pick_rows(rank):
    epd = rank.shape[1]
    r = jnp.arange(epd * CAP)
    rep = (r[:, None] // CAP == jnp.arange(epd)[None, :]).astype(jnp.bfloat16)
    full = jnp.einsum('re,set->srt', rep, rank, preferred_element_type=jnp.float32)
    return (full == (r % CAP).astype(jnp.float32)[None, :, None]).astype(jnp.bfloat16)


def expert_rows(ublk, sel, we_g, we_u, we_d):
    n, _, d = ublk.shape
    epd = we_g.shape[0]
    xin = jnp.einsum('srt,std->srd', sel, ublk, preferred_element_type=jnp.float32).astype(jnp.bfloat16)
    xin = xin.reshape(n, epd, CAP, d).transpose(1, 0, 2, 3).reshape(epd, n * CAP, d)
    hg = jnp.einsum('ecd,edf->ecf', xin, we_g, preferred_element_type=jnp.float32)
    hu = jnp.einsum('ecd,edf->ecf', xin, we_u, preferred_element_type=jnp.float32)
    hh = lax.optimization_barrier((jax.nn.silu(hg) * hu).astype(jnp.bfloat16))
    yo = jnp.einsum('ecf,efd->ecd', hh, we_d, preferred_element_type=jnp.float32).astype(jnp.bfloat16)
    return yo.reshape(epd, n, CAP, d)


def weights(g, rank):
    ne, _ = g.shape
    r = jnp.arange(ne * CAP)
    rep = (r[:, None] // CAP == jnp.arange(ne)[None, :]).astype(jnp.bfloat16)
    full = jnp.einsum('et,re->tr', rank, rep, preferred_element_type=jnp.float32)
    sel = (full == (r % CAP).astype(jnp.float32)[None, :])[None]
    w = jnp.einsum('pet,re->ptr', jnp.stack(split3(g)), rep, preferred_element_type=jnp.float32)
    return jnp.where(sel, w, 0.0).astype(jnp.bfloat16)


def solution(mesh):
    ncp = mesh.shape['cp']
    ndev = mesh.shape['b'] * ncp
    tok = P(('dp', 'b'), 'cp', None)
    rep = P()
    exs = P(('b', 'cp'), None, None)

    def layer(x, ids, g_attn, wq, wk, wv, wo, g_ffn, w1, w3, w2, g_moe, wr, we_g, we_u, we_d):
        bd, sd, d = x.shape
        nh = wq.shape[1] // HEAD
        epd = we_g.shape[0]
        nexp = epd * ndev
        nb = ndev // ncp
        ci = lax.axis_index('cp')
        bi = lax.axis_index('b')
        u = rms_norm(x, g_moe).reshape(bd * sd, d)
        info, zero = gates(u, ids, wr, nexp)
        info = lax.all_gather(info, ('b', 'cp'), axis=0, tiled=False)
        info, usend, xa = lax.optimization_barrier((info, u, x))
        uall = lax.all_gather(usend, ('b', 'cp'), axis=0, tiled=False)
        pos = ci * sd + jnp.arange(sd)
        n = rms_norm(xa, g_attn)
        q = rope(proj(n, wq).reshape(bd, sd, nh, HEAD), pos).reshape(bd, sd, nh, 1, HEAD).transpose(0, 2, 3, 1, 4)
        kv = jnp.stack([rope(proj(n, wk).reshape(bd, sd, nh, HEAD), pos), proj(n, wv).reshape(bd, sd, nh, HEAD)])
        mx = jnp.full((bd, nh, 1, sd), -1e30, jnp.float32)
        den = jnp.zeros((bd, nh, 1, sd), jnp.float32)
        acc = jnp.zeros((bd, nh, 1, sd, HEAD), jnp.float32)
        mx, den, acc = attend(q, kv[0], kv[1], pos, pos, mx, den, acc)
        for step in range(1, ncp):
            kv = lax.ppermute(kv, 'cp', [(j, j + 1) for j in range(step - 1, ncp - 1)])
            kpos = ((ci - step) % ncp) * sd + jnp.arange(sd)
            mx, den, acc = attend(q, kv[0], kv[1], pos, kpos, mx, den, acc)
        o = (acc / den[..., None]).astype(jnp.bfloat16).transpose(0, 3, 1, 2, 4).reshape(bd, sd, nh * HEAD)
        y = (x.astype(jnp.float32) + proj(o, wo).astype(jnp.float32)).astype(jnp.bfloat16)

        g, rank = tables(info, bi * (ncp * epd), ncp * epd)
        g = g.reshape(nb, ncp, ncp * epd, sd)
        rank = rank.reshape(nb, ncp, ncp * epd, sd)
        mine = lax.dynamic_slice_in_dim(rank, ci * epd, epd, axis=2)
        gcol = lax.dynamic_index_in_dim(g, ci, axis=1, keepdims=False)
        rcol = lax.dynamic_index_in_dim(rank, ci, axis=1, keepdims=False)
        peers = [jnp.bitwise_xor(ci, k) for k in range(ncp)]
        order = jnp.asarray(ORDER, jnp.int32)
        blks = [order[bi, i] for i in range(nb)]
        uall = uall.reshape(nb, ncp, sd, d)

        def row_picks(i):
            return pick_rows(lax.dynamic_index_in_dim(mine, blks[i], axis=0, keepdims=False))

        def row_weights(i):
            gi = lax.dynamic_index_in_dim(gcol, blks[i], axis=0, keepdims=False)
            ri = lax.dynamic_index_in_dim(rcol, blks[i], axis=0, keepdims=False)
            gi = jnp.concatenate([lax.dynamic_slice_in_dim(gi, p * epd, epd, axis=0) for p in peers], axis=0)
            ri = jnp.concatenate([lax.dynamic_slice_in_dim(ri, p * epd, epd, axis=0) for p in peers], axis=0)
            return weights(gi, ri).reshape(3 * sd, ncp * epd * CAP)

        def work(ua, i):
            blk = lax.dynamic_index_in_dim(ua, blks[i], axis=0, keepdims=False)
            return expert_rows(blk, sels[i], we_g, we_u, we_d)

        def send(yo):
            got = []
            for k in range(ncp):
                part = lax.dynamic_index_in_dim(yo, peers[k], axis=1, keepdims=False).reshape(epd * CAP, d)
                if k:
                    part = lax.ppermute(part, 'cp', [(j, j ^ k) for j in range(ncp)])
                got.append(part)
            return got

        def total(got, i):
            rows = lax.optimization_barrier(jnp.concatenate(got, axis=0))
            p = lax.optimization_barrier(jnp.dot(ws[i], rows, preferred_element_type=jnp.float32)).reshape(3, sd, d)
            return p[0] + p[1] + p[2]

        tie = lax.optimization_barrier

        def up(v, step):
            return lax.ppermute(v, 'b', [(j, j + 1) for j in range(step)])

        def down(v, step):
            return lax.ppermute(v, 'b', [(nb - 1 - j, nb - 2 - j) for j in range(step)])

        ws = tie([row_weights(i) for i in range(nb)])
        sels = tie([row_picks(i) for i in range(nb)])
        uall, y, sels, ws = tie((uall, y, sels, ws))
        yo1, uall = tie((work(uall, 0), uall))
        g1 = send(yo1)
        yo2, uall, g1[0] = tie((work(uall, 1), uall, g1[0]))
        g2 = send(yo2)
        p1, uall = tie((total(g1, 0), uall))
        up1, dn1 = up(p1, 1), down(p1, 1)
        yo3, uall, g2[0] = tie((work(uall, 2), uall, g2[0]))
        g3 = send(yo3)
        p2, uall = tie((total(g2, 1), uall))
        yo4, g3[0], p2 = tie((work(uall, 3), g3[0], p2))
        g4 = send(yo4)
        a2, b2, g3[0] = tie((p2 + up1, p2 + dn1, g3[0]))
        up2, dn2 = up(a2, 2), down(b2, 2)
        p3, y = tie((total(g3, 2), y))
        zf = rms_norm(y, g_ffn)
        hh = (jax.nn.silu(jnp.dot(zf, w1, preferred_element_type=jnp.float32)) * jnp.dot(zf, w3, preferred_element_type=jnp.float32)).astype(jnp.bfloat16)
        a3 = jnp.where(bi == 2, p1, p3) + up2
        b3 = jnp.where(bi == 1, p1, p3) + dn2
        hh, a3, b3, g4[0] = tie((hh, a3, b3, g4[0]))
        up3, dn3 = up(a3, 3), down(b3, 3)
        p4 = total(g4, 3)
        f = lax.optimization_barrier(proj(hh, w2))
        m = (p4 + zero * u.astype(jnp.float32)) + up3 + dn3
        h = y.astype(jnp.float32) + f.astype(jnp.float32) + m.reshape(bd, sd, d)
        return h.astype(jnp.bfloat16)

    return jax.shard_map(layer, mesh=mesh, in_specs=(tok, tok, rep, rep, rep, rep, rep, rep, rep, rep, rep, rep, rep, exs, exs, exs), out_specs=tok, check_vma=False)
```
